32 devices in a mesh: mem: 16 (over z, y, core), band: 2 (over x).
Axes of the slice: x: 2, y: 2, z: 4, core: 2. Of those that a mesh axis runs over, the one named last changes fastest.
Arguments:
- ensemble: bfloat16 [16, 12, 32, 128], P('mem', None, 'band'), may hold values from -6 to 6
- alpha: float32 [16, 12, 32, 128], P('mem', None, 'band'), may hold values from -6 to 6
- lat_lower: int32 [96], P('band'), may hold values from -1 to 15, as said below
- lat_weight: float32 [96], P('band'), may hold values from 0 to 1
- background: float32 [12, 32, 1152], P(None, ('band', 'mem')), may hold values from -6 to 6
- obs_cell: int32 [32, 256], P(('band', 'mem')), may hold values from 0 to 1151
- obs_value: float32 [12, 32, 256], P(None, ('band', 'mem')), may hold values from -6 to 6
- obs_precision: float32 [32, 256], P(('band', 'mem')), may hold values from 1 to 10
Outputs:
- advected: float32 [12, 32, 1152], P(None, ('band', 'mem'))
- gradient: float32 [16, 12, 32, 128], P('mem', None, 'band')
The draws below stay inside these ranges and needn't reach their ends.
Inputs may be any that keep to these rules, and one draw needn't show every extreme that they name: `lat_lower`: fine rows of the first band use lower rows from 0, those of the last band up to 14 of their band, so that their upper row reaches 15; other bands reach -1 and 15. `obs_cell`: the cell is r * 24 + c for fine row r and column c within the tile.
All inputs are finite; a program needn't handle non-finite values.
Results may differ from the reference program's by a relative error of at most 0.0004.
Values sent between devices are 32-bit elements; how exact they have to be, the bound alone decides.
A program may use at most 64 MiB of HBM per device.

```python
import math
import jax
import jax.numpy as jnp
from jax import lax

LEV = 12
CLAT_B = 16
NOBS = 256
MEMBERS = 16
CLAT = 32
CLON = 128
FLAT_B = 48
FLON_T = 24
FLAT = 96
FLON = 384
TILES = 32
TILE_CELLS = 1152
N_MEM = 16
N_BAND = 2


def draw_lat_lower(key, part):
    fine_index = jnp.arange(FLAT, dtype=jnp.int32)
    inner = fine_index % FLAT_B
    band_index = fine_index // FLAT_B
    jitter = jax.random.randint(key, (FLAT,), 0, 2, dtype=jnp.int32)
    jitter = jnp.where(inner == 0, 0, jnp.where(inner == FLAT_B - 1, 1, jitter))
    lower_row = inner * CLAT_B // FLAT_B - 1 + jitter
    lower_row = jnp.where(band_index == 0, jnp.maximum(lower_row, 0), lower_row)
    lower_row = jnp.where(band_index == FLAT // FLAT_B - 1, jnp.minimum(lower_row, CLAT_B - 2), lower_row)
    return lower_row.astype(jnp.int32)


def touch_ends(values, stream_key, smallest, high):
    longest = values.shape.index(max(values.shape))
    spots = []
    for shift in (0, 1):
        where = [jax.random.randint(jax.random.fold_in(stream_key, axis), (), 0, length) for axis, length in enumerate(values.shape)]
        where[longest] = (where[longest] + shift) % values.shape[longest]
        spots.append(tuple(where))
    return values.at[spots[0]].set(smallest).at[spots[1]].set(high)


def level_of(key, extent, shards, least, largest):
    def one(axis_at, parts):
        steps = jax.random.uniform(jax.random.fold_in(jax.random.fold_in(key, 6), axis_at), (parts,), jnp.float32, least / len(shards), largest / len(shards))
        return jnp.repeat(jnp.exp(steps), extent[axis_at] // parts).reshape((-1,) + (1,) * (len(extent) - axis_at - 1))

    level = one(*shards[0])
    for cut in shards[1:]:
        level = level * one(*cut)
    return level


def centred(stream_key, shape, scale, most, cuts=(), kind=jnp.bfloat16):
    result = scale * jax.random.normal(stream_key, shape, jnp.float32)
    if cuts:
        result = result * level_of(stream_key, shape, cuts, -0.22, 0.18)
    return jnp.clip(result, -most, most).astype(kind)


def setup_inputs(seed: int = 0) -> dict:
    key_of = jax.random.split(jax.random.key(seed), 9)
    ensemble = centred(key_of[0], (MEMBERS, LEV, CLAT, CLON), 1.0, 6.0, ((0, 16), (2, 2)))
    alpha = centred(key_of[1], (MEMBERS, LEV, CLAT, CLON), 1.0, 6.0, ((0, 16), (2, 2)), jnp.float32)
    lat_lower = draw_lat_lower(jax.random.fold_in(key_of[8], 71), 0)
    lat_weight = jnp.clip(1.0 * jax.random.uniform(key_of[3], (FLAT,), jnp.float32) ** level_of(key_of[3], (FLAT,), ((0, 2),), -0.2, 0.2), 0.0, 1.0)
    background = centred(key_of[4], (LEV, TILES, TILE_CELLS), 1.0, 6.0, ((1, 32),), jnp.float32)
    obs_cell = touch_ends(jax.random.randint(key_of[5], (TILES, NOBS), 0, TILE_CELLS), jax.random.fold_in(key_of[5], 1), 0, TILE_CELLS - 1).astype(jnp.int32)
    obs_value = centred(key_of[6], (LEV, TILES, NOBS), 1.0, 6.0, ((1, 32),), jnp.float32)
    obs_precision = jnp.clip(jnp.exp(math.log(10.0) - 2.3025851 * jax.random.uniform(key_of[7], (TILES, NOBS), jnp.float32) ** level_of(key_of[7], (TILES, NOBS), ((0, 32),), -0.2, 0.2)), 1.0, 10.0)
    return {"ensemble": ensemble, "alpha": alpha, "lat_lower": lat_lower, "lat_weight": lat_weight, "background": background, "obs_cell": obs_cell, "obs_value": obs_value, "obs_precision": obs_precision}


advect_rate = 0.25
highest = lax.Precision.HIGHEST

def smooth_field(grid_field):
    padded = jnp.pad(grid_field, ((0, 0), (0, 0), (1, 1), (0, 0)))
    grid_field = 0.25 * padded[:, :, :-2] + 0.5 * padded[:, :, 1:-1] + 0.25 * padded[:, :, 2:]
    return 0.25 * jnp.roll(grid_field, 1, 3) + 0.5 * grid_field + 0.25 * jnp.roll(grid_field, -1, 3)

def latitude_table(lat_lower, lat_weight):
    fine_index = jnp.arange(FLAT, dtype=jnp.int32)
    lower_row = fine_index // FLAT_B * CLAT_B + lat_lower
    coarse = jnp.arange(CLAT, dtype=jnp.int32)
    weight = lat_weight[:, None]
    return (1.0 - weight) * (coarse[None, :] == lower_row[:, None]) + weight * (coarse[None, :] == lower_row[:, None] + 1)

def longitude_table(coarse_cols, fine_cols):
    fine_ratio = fine_cols // coarse_cols
    fine_index = jnp.arange(fine_cols, dtype=jnp.int32)
    numerator = 2 * fine_index + 1 + fine_ratio
    upper_col = numerator // (2 * fine_ratio)
    fraction = (numerator % (2 * fine_ratio)).astype(jnp.float32) / (2 * fine_ratio)
    coarse = jnp.arange(coarse_cols, dtype=jnp.int32)[:, None]
    low_col = (upper_col - 1) % coarse_cols
    high_col = upper_col % coarse_cols
    return (1.0 - fraction)[None, :] * (coarse == low_col[None, :]) + fraction[None, :] * (coarse == high_col[None, :])

def reference(ensemble, alpha, lat_lower, lat_weight, background, obs_cell, obs_value, obs_precision):
    member_scale = 1.0 / math.sqrt(MEMBERS - 1)
    members_f = ensemble.astype(jnp.float32)
    increment = lax.optimization_barrier(jnp.sum(smooth_field(alpha) * members_f, axis=0)) * member_scale
    lat_table = latitude_table(lat_lower, lat_weight)
    lon_table = longitude_table(CLON, FLON)
    fine_grid = background.reshape(LEV, N_BAND, N_MEM, FLAT_B, FLON_T).transpose(0, 1, 3, 2, 4).reshape(LEV, FLAT, FLON)
    indices = jnp.broadcast_to(obs_cell[None], (LEV, TILES, NOBS))

    def fine_model(incr):
        lat_rows = jnp.einsum('ik,lkc->lic', lat_table, incr, precision=highest)
        fine_incr = jnp.einsum('lic,cj->lij', lat_rows, lon_table, precision=highest)
        fine_state = fine_grid + fine_incr
        lon_slope = 0.5 * (jnp.roll(fine_state, -1, 2) - jnp.roll(fine_state, 1, 2))
        moved = fine_state - advect_rate * fine_state * lon_slope
        return moved.reshape(LEV, N_BAND, FLAT_B, N_MEM, FLON_T).transpose(0, 1, 3, 2, 4).reshape(LEV, TILES, TILE_CELLS)

    def observed_of(incr):
        return jnp.take_along_axis(fine_model(incr), indices, axis=2)
    advected = fine_model(increment)
    observed, pullback = jax.vjp(observed_of, increment)
    weighted = obs_precision[None] * (observed - obs_value)
    coarse_gradient = pullback(weighted)[0]
    gradient = smooth_field(members_f * coarse_gradient[None] * member_scale)
    return (advected, gradient)
```

```python
import functools
import math

import jax
import jax.numpy as jnp
from jax import lax
from jax.experimental import pallas as pl
from jax.experimental.pallas import tpu as pltpu
from jax.sharding import PartitionSpec as P

advect_rate = 0.25
LANES = 128
f32 = jnp.float32
bf16 = jnp.bfloat16


def split2(x):
    hi = x.astype(bf16)
    lo = (x - hi.astype(f32)).astype(bf16)
    return hi, lo


def dims(a, b, ca, cb):
    return lax.dot_general(a, b, (((ca,), (cb,)), ((), ())), preferred_element_type=f32)


def smooth_lon(x):
    n = x.shape[1]
    return 0.25 * pltpu.roll(x, 1, 1) + 0.5 * x + 0.25 * pltpu.roll(x, n - 1, 1)


def kernel(
    cfg,
    ens_ref,
    alpha_ref,
    low_ref,
    wt_ref,
    bg_ref,
    cell_ref,
    val_ref,
    prec_ref,
    adv_ref,
    grad_ref,
    ensf,
    edge_send,
    edge_recv,
    partial_rows,
    send1,
    recv1,
    sum1,
    place,
    table_hi,
    table_lo,
    frame_rows,
    frame_recv,
    send2,
    recv2,
    merged,
    coarse,
    edge_ss,
    edge_rs,
    frame_ss,
    frame_rs,
    ss1,
    rs1,
    ss2,
    rs2,
    bg_recv,
    bg_ss,
    bg_rs,
):
    n, nb, lev, rows, lon, fine_rows, fine_cols, scale = cfg
    block = lon // n
    frame = block + 2
    ratio = fine_cols // block
    cells = fine_rows * fine_cols
    wrows = recv1.shape[1]
    per = LANES // frame
    order = list(range(1, rows - 1)) + [-1, 0, rows - 1, rows]
    slot = {k: i for i, k in enumerate(order)}
    up_at = (rows - 2) * lev
    down_at = rows * lev
    groups = partial_rows.shape[0] // LANES
    me = lax.axis_index("mem")
    band = lax.axis_index("band")
    has_up = band > 0
    has_down = band < nb - 1

    barrier = pltpu.get_barrier_semaphore()

    def greet(o, c):
        pl.semaphore_signal(barrier, inc=1, device_id={"mem": lax.rem(me + o, n)})
        return c

    lax.fori_loop(1, n, greet, 0)

    @pl.when(has_up)
    def _():
        pl.semaphore_signal(barrier, inc=1, device_id={"band": band - 1})

    @pl.when(has_down)
    def _():
        pl.semaphore_signal(barrier, inc=1, device_id={"band": band + 1})

    ensf[...] = ens_ref[...].astype(f32)

    def row(ref, k):
        parts = [ref.at[t][pl.ds(k, lev, stride=rows), :] for t in range(lon // LANES)]
        return parts[0] if len(parts) == 1 else jnp.concatenate(parts, axis=1)

    for side, ks in ((0, (0, 1)), (1, (rows - 1, rows - 2))):
        edge_send[side, 0, 0:lev, :] = row(alpha_ref, ks[0])
        edge_send[side, 1, 0:lev, :] = row(alpha_ref, ks[1])
        edge_send[side, 2, 0:lev, :] = row(ensf, ks[0])

    if nb == 2:
        pl.semaphore_wait(barrier, n)
    else:
        pl.semaphore_wait(barrier, n - 1 + has_up.astype(jnp.int32) + has_down.astype(jnp.int32))

    def edge_copy(side):
        return pltpu.make_async_remote_copy(
            src_ref=edge_send.at[side],
            dst_ref=edge_recv.at[1 - side],
            send_sem=edge_ss.at[side],
            recv_sem=edge_rs.at[1 - side],
            device_id={"band": band - 1 if side == 0 else band + 1},
        )

    def frame_copy(side):
        at = up_at if side == 0 else down_at
        return pltpu.make_async_remote_copy(
            src_ref=frame_rows.at[pl.ds(at, 2 * lev), :],
            dst_ref=frame_recv.at[1 - side],
            send_sem=frame_ss.at[side],
            recv_sem=frame_rs.at[1 - side],
            device_id={"band": band - 1 if side == 0 else band + 1},
        )

    def start_band(copy, recv):
        for side, has in ((0, has_up), (1, has_down)):

            @pl.when(has)
            def _():
                copy(side).start()

            @pl.when(jnp.logical_not(has))
            def _():
                recv[side] = jnp.zeros(recv.shape[1:], f32)

    def wait_band(copy):
        for side, has in ((0, has_up), (1, has_down)):

            @pl.when(has)
            def _():
                copy(side).wait_send()
                copy(1 - side).wait_recv()

    start_band(edge_copy, edge_recv)

    def bg_copy(side):
        return pltpu.make_async_remote_copy(
            src_ref=bg_ref,
            dst_ref=bg_recv.at[1 - side],
            send_sem=bg_ss.at[side],
            recv_sem=bg_rs.at[1 - side],
            device_id={"mem": lax.rem(me + (n - 1 if side == 0 else 1), n)},
        )

    bg_copy(0).start()
    bg_copy(1).start()

    fr = lax.broadcasted_iota(jnp.int32, (fine_rows, cells), 0)
    fc = lax.broadcasted_iota(jnp.int32, (fine_rows, cells), 1)
    pick = (fc // fine_cols == fr).astype(bf16)
    w_hi = wt_ref[...].astype(bf16)
    rest = wt_ref[...] - w_hi.astype(f32)
    w_mid = rest.astype(bf16)
    w_lo = (rest - w_mid.astype(f32)).astype(bf16)
    low_b = low_ref[...].astype(f32).astype(bf16)
    rowvec = jnp.concatenate([jnp.broadcast_to(v, (8, fine_rows)) for v in (w_hi.astype(f32), w_mid.astype(f32), w_lo.astype(f32), low_b.astype(f32))], axis=0)
    spread = dims(rowvec.astype(bf16), pick, 1, 0)
    wcell = spread[0:1] + spread[8:9] + spread[16:17]
    lcell = spread[24:25].astype(jnp.int32)
    cell = lax.broadcasted_iota(jnp.int32, (1, cells), 1)
    col = cell % fine_cols

    def lon_parts(shift):
        num = 2 * (col + shift) + 1 + ratio
        return num // (2 * ratio), (num % (2 * ratio)).astype(f32) / (2 * ratio)

    q0, f0 = lon_parts(0)
    qn, fn = lon_parts(1)
    qp, fp = lon_parts(-1)
    chunk = 32

    def table_step(i, c):
        kap = lax.broadcasted_iota(jnp.int32, (chunk, 1), 0) + i * chunk
        lane = kap % LANES
        k = (kap // LANES) * per + lane // frame
        w = lane % frame
        ok = lane < per * frame
        k = jnp.where(ok, k, -5)
        w = jnp.where(ok, w, -5)
        latv = jnp.where(k == lcell + 1, 1.0 - wcell, 0.0) + jnp.where(k == lcell + 2, wcell, 0.0)

        def lonv(q, f):
            return jnp.where(w == q, 1.0 - f, 0.0) + jnp.where(w == q + 1, f, 0.0)

        at = pl.ds(pl.multiple_of(i * chunk, chunk), chunk)
        hi, lo = split2(latv * lonv(q0, f0))
        table_hi[at, 0:cells] = hi
        table_lo[at, 0:cells] = lo
        hi, lo = split2(latv * (0.5 * (lonv(qn, fn) - lonv(qp, fp))))
        table_hi[at, cells : 2 * cells] = hi
        table_lo[at, cells : 2 * cells] = lo
        return c

    lax.fori_loop(0, table_hi.shape[0] // chunk, table_step, 0)

    nobs = cell_ref.shape[1]
    prec = prec_ref[...]
    lhs = jnp.concatenate([prec * val_ref[:, 0, :], prec, jnp.zeros((16 - lev - 1, nobs), f32)], axis=0)
    l_hi = lhs.astype(bf16).astype(f32)
    l_mid = (lhs - l_hi).astype(bf16).astype(f32)
    l_lo = lhs - l_hi - l_mid
    l3 = jnp.concatenate([l_hi, l_mid, l_lo], axis=0).astype(bf16)
    hot = (lax.broadcasted_iota(jnp.int32, (cells, nobs), 0) == cell_ref[...]).astype(f32).astype(bf16)
    obs = dims(l3, hot, 1, 1)
    obs = obs[0:16] + obs[16:32] + obs[32:48]
    obs_b = obs[0:lev]
    obs_a = obs[lev : lev + 1]
    partial_rows[...] = jnp.zeros(partial_rows.shape, f32)
    frame_rows[...] = jnp.zeros(frame_rows.shape, f32)
    send1[...] = jnp.zeros(send1.shape, f32)
    send2[...] = jnp.zeros(send2.shape, f32)
    back = bg_ref[:, 0, :]
    for side in (0, 1):
        bg_copy(side).wait()
    from_left, from_right = bg_recv[0, :, 0, :], bg_recv[1, :, 0, :]
    before = jnp.where(col == 0, pltpu.roll(from_left, cells - fine_cols + 1, 1), pltpu.roll(back, 1, 1))
    after = jnp.where(
        col == fine_cols - 1, pltpu.roll(from_right, fine_cols - 1, 1), pltpu.roll(back, cells - 1, 1)
    )
    back_slope = 0.5 * (after - before)

    wait_band(edge_copy)

    def alpha_row(k):
        if k < 0:
            return edge_recv[0, -1 - k, 0:lev, :]
        if k >= rows:
            return edge_recv[1, k - rows, 0:lev, :]
        return row(alpha_ref, k)

    def ens_row(k):
        if k < 0:
            return edge_recv[0, 2, 0:lev, :]
        if k >= rows:
            return edge_recv[1, 2, 0:lev, :]
        return row(ensf, k)

    for k in range(-1, rows + 1):
        s = 0.25 * alpha_row(k - 1) + 0.5 * alpha_row(k) + 0.25 * alpha_row(k + 1)
        partial_rows[slot[k] * lev : (slot[k] + 1) * lev, :] = smooth_lon(s) * ens_row(k) * scale

    for g in range(groups):
        for t in range(lon // LANES):
            piece = partial_rows[g * LANES : (g + 1) * LANES, t * LANES : (t + 1) * LANES].T
            send1[pl.ds(groups * (t * LANES + 1) + g, LANES, stride=groups), :] = piece
    send1[0:groups, :] = send1[groups * lon : groups * (lon + 1), :]
    send1[groups * (lon + 1) : groups * (lon + 2), :] = send1[groups : 2 * groups, :]

    step = groups * block

    def copy1(dst):
        return pltpu.make_async_remote_copy(
            src_ref=send1.at[pl.ds(pl.multiple_of(dst * step, step), wrows), :],
            dst_ref=recv1.at[me],
            send_sem=ss1.at[dst],
            recv_sem=rs1.at[me],
            device_id={"mem": dst},
        )

    def copy2(dst):
        return pltpu.make_async_remote_copy(
            src_ref=send2,
            dst_ref=recv2.at[me],
            send_sem=ss2.at[dst],
            recv_sem=rs2.at[me],
            device_id={"mem": dst},
        )

    def start_all(copy):
        def go(o, c):
            copy(lax.rem(me + o, n)).start()
            return c

        lax.fori_loop(1, n, go, 0)

    def wait_all(copy, recv, ss, rs):
        def go(o, c):
            src = lax.rem(me + o, n)
            pltpu.make_async_copy(recv.at[src], recv.at[src], rs.at[src]).wait()
            copy(src).wait_send()
            return c

        lax.fori_loop(1, n, go, 0)

    start_all(copy1)
    recv1[me] = send1[pl.ds(pl.multiple_of(me * step, step), wrows), :]
    wait_all(copy1, recv1, ss1, rs1)
    total = recv1[0]
    for s in range(1, n):
        total = total + recv1[s]
    sum1[...] = total
    fr_pad = wrows // groups
    for g in range(groups):
        win = sum1[pl.ds(g, fr_pad, stride=groups), :]
        win = jnp.concatenate([win, jnp.zeros((LANES - fr_pad, LANES), f32)], axis=0)
        place[g * LANES : (g + 1) * LANES, :] = win.T

    lane16 = lax.broadcasted_iota(jnp.int32, (lev, LANES), 1)
    tiles = table_hi.shape[0] // LANES
    x_tiles = []
    for t in range(tiles):
        acc = jnp.zeros((lev, LANES), f32)
        for j in range(per):
            k = t * per + j - 1
            if k > rows:
                break
            piece = place[slot[k] * lev : (slot[k] + 1) * lev, :]
            if j:
                piece = pltpu.roll(piece, j * frame, 1)
            acc = jnp.where((lane16 >= j * frame) & (lane16 < (j + 1) * frame), piece, acc)
        x_tiles.append(acc)
    x = jnp.concatenate(x_tiles, axis=1)
    x = jnp.concatenate([x, jnp.zeros((16 - lev, x.shape[1]), f32)], axis=0)
    x_hi = x.astype(bf16).astype(f32)
    x2 = jnp.concatenate([x_hi, x - x_hi], axis=0).astype(bf16)
    y = dims(x2, table_hi[...], 1, 0)
    y = y[0:16] + y[16:32] + dims(x_hi.astype(bf16), table_lo[...], 1, 0)

    state = back + y[0:lev, 0:cells]
    slope = y[0:lev, cells : 2 * cells] + back_slope
    factor = 1.0 - advect_rate * slope
    moved = state * factor
    adv_ref[:, 0, :] = moved
    cot = obs_a * moved - obs_b
    uv = jnp.concatenate([cot * factor, (-advect_rate) * (state * cot)], axis=1)
    uv = jnp.concatenate([uv, jnp.zeros((16 - lev, 2 * cells), f32)], axis=0)
    uv_hi = uv.astype(bf16).astype(f32)
    uv2 = jnp.concatenate([uv_hi, uv - uv_hi], axis=0).astype(bf16)
    gr = dims(uv2, table_hi[...], 1, 1)
    gr = gr[0:16] + gr[16:32] + dims(uv_hi.astype(bf16), table_lo[...], 1, 1)
    for t in range(tiles):
        tile = gr[0:lev, t * LANES : (t + 1) * LANES]
        for j in range(per):
            k = t * per + j - 1
            if k > rows:
                break
            piece = tile if j == 0 else pltpu.roll(tile, LANES - j * frame, 1)
            piece = jnp.where(lane16 < frame, piece, 0.0)
            frame_rows[slot[k] * lev : (slot[k] + 1) * lev, :] = piece

    start_band(frame_copy, frame_recv)
    wait_band(frame_copy)
    frame_rows[up_at : up_at + 2 * lev, :] += frame_recv[0]
    frame_rows[down_at : down_at + 2 * lev, :] += frame_recv[1]
    for g in range(groups):
        send2[pl.ds(g, fr_pad, stride=groups), :] = frame_rows[g * LANES : (g + 1) * LANES, :].T[0:fr_pad]
    start_all(copy2)
    recv2[me] = send2[...]
    wait_all(copy2, recv2, ss2, rs2)

    over = wrows - step
    for d in range(n):
        merged[d * step : (d + 1) * step, :] = recv2[d, 0:step, :]
    for d in range(n):
        e = (d + 1) % n
        merged[e * step : e * step + over, :] += recv2[d, step:wrows, :]
    for g in range(groups):
        for t in range(lon // LANES):
            piece = merged[pl.ds(groups * t * LANES + g, LANES, stride=groups), :].T
            coarse[g * LANES : (g + 1) * LANES, t * LANES : (t + 1) * LANES] = piece

    def weighted(k):
        cg = coarse[slot[k] * lev : (slot[k] + 1) * lev, :]
        return ens_row(k) * pltpu.roll(cg, lon - 1, 1) * scale

    a, b = weighted(-1), weighted(0)
    for k in range(rows):
        c = weighted(k + 1)
        z = smooth_lon(0.25 * a + 0.5 * b + 0.25 * c)
        for t in range(lon // LANES):
            grad_ref.at[t][pl.ds(k, lev, stride=rows), :] = z[:, t * LANES : (t + 1) * LANES]
        a, b = b, c


def up_to(x, m):
    return -(-x // m) * m


def to_tiles(x):
    return x.reshape(-1, x.shape[3] // LANES, LANES).swapaxes(0, 1)


def shards(ensemble, alpha, lat_lower, lat_weight, background, obs_cell, obs_value, obs_precision):
    n, nb = lax.axis_size("mem"), lax.axis_size("band")
    members, lev, rows, lon = ensemble.shape
    fine_rows = lat_lower.shape[0]
    cells = background.shape[2]
    scale = 1.0 / math.sqrt(members * n - 1)
    block = lon // n
    frame = block + 2
    groups = up_to((rows + 2) * lev, LANES) // LANES
    wrows = up_to(groups * frame, 8 * groups // math.gcd(8, groups))
    per = LANES // frame
    kaps = -(-(rows + 2) // per) * LANES
    cfg = (n, nb, lev, rows, lon, fine_rows, cells // fine_rows, scale)
    levp = up_to(lev, 8)
    dma = pltpu.SemaphoreType.DMA
    vm = pl.BlockSpec(memory_space=pltpu.VMEM)
    advected, gradient = pl.pallas_call(
        functools.partial(kernel, cfg),
        out_shape=(
            jax.ShapeDtypeStruct(background.shape, f32),
            jax.ShapeDtypeStruct((lon // LANES, lev * rows, LANES), f32),
        ),
        in_specs=[vm] * 8,
        out_specs=(vm, vm),
        scratch_shapes=[
            pltpu.VMEM((lon // LANES, lev * rows, LANES), f32),
            pltpu.VMEM((2, 3, levp, lon), f32),
            pltpu.VMEM((2, 3, levp, lon), f32),
            pltpu.VMEM((groups * LANES, lon), f32),
            pltpu.VMEM((groups * lon + wrows, LANES), f32),
            pltpu.VMEM((n, wrows, LANES), f32),
            pltpu.VMEM((wrows, LANES), f32),
            pltpu.VMEM((groups * LANES, LANES), f32),
            pltpu.VMEM((kaps, 2 * cells), bf16),
            pltpu.VMEM((kaps, 2 * cells), bf16),
            pltpu.VMEM((groups * LANES, LANES), f32),
            pltpu.VMEM((2, 2 * lev, LANES), f32),
            pltpu.VMEM((wrows, LANES), f32),
            pltpu.VMEM((n, wrows, LANES), f32),
            pltpu.VMEM((groups * lon, LANES), f32),
            pltpu.VMEM((groups * LANES, lon), f32),
            dma((2,)),
            dma((2,)),
            dma((2,)),
            dma((2,)),
            dma((n,)),
            dma((n,)),
            dma((n,)),
            dma((n,)),
            pltpu.VMEM((2,) + background.shape, f32),
            dma((2,)),
            dma((2,)),
        ],
        compiler_params=pltpu.CompilerParams(collective_id=0, has_side_effects=True, vmem_limit_bytes=48 * 2**20),
    )(
        to_tiles(ensemble),
        to_tiles(alpha),
        lat_lower.reshape(1, fine_rows),
        lat_weight.reshape(1, fine_rows),
        background,
        obs_cell,
        obs_value,
        obs_precision,
    )
    return advected, gradient.swapaxes(0, 1).reshape(members, lev, rows, lon)


def solution(mesh):
    return jax.shard_map(
        shards,
        mesh=mesh,
        in_specs=(
            P("mem", None, "band", None),
            P("mem", None, "band", None),
            P("band"),
            P("band"),
            P(None, ("band", "mem"), None),
            P(("band", "mem"), None),
            P(None, ("band", "mem"), None),
            P(("band", "mem"), None),
        ),
        out_specs=(P(None, ("band", "mem"), None), P("mem", None, "band", None)),
        check_vma=False,
    )
```
